32 devices in a mesh: leaf: 8 (over z, y), blk: 4 (over x, core).
Axes of the slice: x: 2, y: 2, z: 4, core: 2. Of those that a mesh axis runs over, the one named last changes fastest.
Arguments:
- src_pos: int32 [4, 2097152], P('blk', 'leaf'), may hold values from 0 to 8388607, as said below
- strengths: float32 [2, 4, 2097152], P(None, 'blk', 'leaf'), may hold values from -0.001953125 to 0.001953125
- tgt_pos: int32 [8388608], P(('leaf', 'blk')), may hold values from 0 to 201326591, as said below
Outputs:
- field: float32 [2, 8388608], P(None, ('leaf', 'blk'))
The draws below stay inside these ranges and needn't reach their ends.
Inputs may be any that keep to these rules, and one draw needn't show every extreme that they name: `src_pos`: row q holds 16384 runs of 128 cells; run b lies in the 128 cells from (q * 16384 + b) * 128 on. `tgt_pos`: the ticks held by index k of leaf, at every index of blk, come in 2048 runs of 128; run j lies in the 12288 ticks from (j * 8 + r) * 12288 on, where r is k with its 3 binary digits in reverse order.
All inputs are finite; a program needn't handle non-finite values.
Results may differ from the reference program's by a relative error of at most 0.0003.
Values sent between devices are 32-bit elements; how exact they have to be, the bound alone decides.
A program may use at most 128 MiB of HBM per device.

```python
import math
import jax
import jax.numpy as jnp
import numpy as np
from jax import lax

R = 16
PER_BOX = 128
TGT_BOX = 128
BOX_CELLS = 128
TOP_TICKS = 201326592
LB = 2048
GROUP_SRC = 2097152
N_LEAF = 8
N_BLK = 4


def draw_src_pos(key, part):
    column_count = N_LEAF * LB * PER_BOX
    row_ids = jnp.arange(N_BLK, dtype=jnp.int32)[:, None]
    columns = jnp.arange(column_count, dtype=jnp.int32)[None, :]
    box_ids = row_ids * (N_LEAF * LB) + columns // PER_BOX
    inside = jax.random.randint(jax.random.fold_in(key, 11), (N_BLK, column_count), 0, BOX_CELLS, dtype=jnp.int32)
    return box_ids * BOX_CELLS + inside


def draw_tgt_pos(key, part):
    per_device = LB * TGT_BOX
    flat_ids = jnp.arange(N_LEAF * N_BLK * per_device, dtype=jnp.int32)
    device = flat_ids // per_device
    leaf_no = device // N_BLK
    run_no = flat_ids % per_device // TGT_BOX
    bit_count = N_LEAF.bit_length() - 1
    reversed_leaf = jnp.zeros_like(leaf_no)
    for bit_no in range(bit_count):
        reversed_leaf = reversed_leaf * 2 + leaf_no // 2 ** bit_no % 2
    box_ticks = TOP_TICKS // (LB * N_LEAF)
    box_ids = run_no * N_LEAF + reversed_leaf
    inside = jax.random.randint(jax.random.fold_in(key, 23), flat_ids.shape, 0, box_ticks, dtype=jnp.int32)
    return box_ids * box_ticks + inside


def level_of(rng, extent, cuts, low, largest):
    def one(position, shards_of):
        heights = jax.random.uniform(jax.random.fold_in(jax.random.fold_in(rng, 6), position), (shards_of,), jnp.float32, low / len(cuts), largest / len(cuts))
        return jnp.repeat(jnp.exp(heights), extent[position] // shards_of).reshape((-1,) + (1,) * (len(extent) - position - 1))

    factor_of = one(*cuts[0])
    for cut in cuts[1:]:
        factor_of = factor_of * one(*cut)
    return factor_of


def gaussian(rng, dims, scale, most, shards=(), kind=jnp.bfloat16):
    drawn = scale * jax.random.normal(rng, dims, jnp.float32)
    if shards:
        drawn = drawn * level_of(rng, dims, shards, -0.22, 0.18)
    return jnp.clip(drawn, -most, most).astype(kind)


def setup_inputs(seed: int = 0) -> dict:
    splits = jax.random.split(jax.random.key(seed), 4)
    src_pos = draw_src_pos(jax.random.fold_in(splits[3], 71), 0)
    strengths = gaussian(splits[1], (2, N_BLK, GROUP_SRC), (N_BLK * GROUP_SRC) ** -0.5, 0.001953125, ((1, 4), (2, 8)), jnp.float32)
    tgt_pos = draw_tgt_pos(jax.random.fold_in(splits[3], 71), 0)
    return {"src_pos": src_pos, "strengths": strengths, "tgt_pos": tgt_pos}


highest_accuracy = lax.Precision.HIGHEST


def node_offsets(box_cells):
    node_index = np.arange(R)
    unit_nodes = (1.0 - np.cos(np.pi * (node_index + 0.5) / R)) / 2.0
    return np.floor(box_cells * unit_nodes).astype(np.int64)


def lagrange_values(node_pos, points):
    basis_rows = []
    for row_node in range(node_pos.shape[0]):
        column = np.ones(points.shape[0])
        for other_node in range(node_pos.shape[0]):
            if other_node != row_node:
                column = column * (points - node_pos[other_node]) / (node_pos[row_node] - node_pos[other_node])
        basis_rows.append(column)
    return np.stack(basis_rows)


def turn_angle(tick_ids, cell_index_list):
    product = tick_ids * cell_index_list
    return product.astype(jnp.float32) * (2.0 * math.pi / 2.0 ** 32)


def leaf_weights(in_box, amounts):
    box_count = in_box.shape[0]
    block_size = min(box_count, 512)
    center = TOP_TICKS // 2
    leaf_nodes = node_offsets(BOX_CELLS)
    node_angles = np.pi * (np.arange(R) + 0.5) / R
    exact_nodes = np.cos(node_angles)
    at_exact = lagrange_values(2.0 * leaf_nodes / BOX_CELLS - 1.0, exact_nodes)
    cheb_at = np.stack([np.cos(degree * node_angles) for degree in range(R)])
    norm_weights = np.where(np.arange(R) == 0, 1.0, 2.0) / R
    coefficients = jnp.asarray(norm_weights[:, None] * (cheb_at @ at_exact.T), jnp.float32)

    def one_block(block_no):
        box_part = lax.dynamic_slice_in_dim(in_box, block_no * block_size, block_size, 0)
        strength_blk = lax.dynamic_slice_in_dim(amounts, block_no * block_size, block_size, 1)
        angles = turn_angle(jnp.int32(center), box_part)
        rotate_re = jnp.cos(angles)
        rotation_imaginary = jnp.sin(angles)
        source_re = rotate_re * strength_blk[0] - rotation_imaginary * strength_blk[1]
        source_im = rotation_imaginary * strength_blk[0] + rotate_re * strength_blk[1]
        scaled = box_part.astype(jnp.float32) * (2.0 / BOX_CELLS) - 1.0
        chebyshev = [jnp.ones_like(scaled), scaled]
        for degree in range(2, R):
            chebyshev.append(2.0 * scaled * chebyshev[-1] - chebyshev[-2])
        moments = jnp.einsum('nbk,xbk->xnb', jnp.stack(chebyshev), jnp.stack([source_re, source_im]), precision=highest_accuracy)
        return jnp.einsum('nt,xnb->xtb', coefficients, moments, precision=highest_accuracy)

    blocks = lax.map(one_block, jnp.arange(box_count // block_size, dtype=jnp.int32))
    mixed_nodes = jnp.transpose(blocks, (1, 2, 0, 3)).reshape(2, R, box_count)
    post_turn = turn_angle(jnp.int32(center), jnp.asarray(leaf_nodes, jnp.int32))
    post_re = jnp.cos(post_turn)[:, None]
    post_im = jnp.sin(post_turn)[:, None]
    out_re = post_re * mixed_nodes[0] + post_im * mixed_nodes[1]
    out_im = post_re * mixed_nodes[1] - post_im * mixed_nodes[0]
    return jnp.stack([out_re, out_im]).reshape(2, R, 1, box_count)


def parent_level(paired, child_ids, tree_level):
    box_a = child_ids.shape[0]
    box_e = child_ids.shape[1]
    box_s = paired.shape[3]
    child_cells = BOX_CELLS * 2 ** tree_level
    child_nodes = node_offsets(child_cells)
    parent_nodes = node_offsets(2 * child_cells)
    inner_cells = np.concatenate([child_nodes, child_nodes + child_cells])
    blend_matrix = jnp.asarray(lagrange_values(parent_nodes / (2.0 * child_cells), inner_cells / (2.0 * child_cells)).reshape(R, 2, R), jnp.float32)
    box_ticks = TOP_TICKS // 2 ** (tree_level + 1)
    centers = child_ids * box_ticks + box_ticks // 2
    pre_turn = turn_angle(centers[:, :, None], jnp.asarray(inner_cells, jnp.int32)[None, None, :]).reshape(box_a, box_e, 2, R)
    pre_re = jnp.cos(pre_turn)[..., None]
    pre_im = jnp.sin(pre_turn)[..., None]
    source = jnp.transpose(paired, (0, 2, 4, 1, 3))[:, :, None]
    rotated_real = pre_re * source[0] - pre_im * source[1]
    rotated_imaginary = pre_im * source[0] + pre_re * source[1]
    accumulated_sum = jnp.einsum('jiw,fpziwd->fjpzd', blend_matrix, jnp.stack([rotated_real, rotated_imaginary]), precision=highest_accuracy)
    post_turn = turn_angle(centers[:, :, None], jnp.asarray(parent_nodes, jnp.int32)[None, None, :])
    post_re = jnp.transpose(jnp.cos(post_turn), (2, 0, 1))[:, :, :, None]
    post_im = jnp.transpose(jnp.sin(post_turn), (2, 0, 1))[:, :, :, None]
    out_re = post_re * accumulated_sum[0] + post_im * accumulated_sum[1]
    out_im = post_re * accumulated_sum[1] - post_im * accumulated_sum[0]
    return jnp.stack([out_re, out_im]).reshape(2, R, box_a * box_e, box_s)


def tree_up(weights, tree_level, first_box):
    box_a = weights.shape[2]
    box_s = weights.shape[3]
    paired = weights.reshape(2, R, box_a, box_s // 2, 2)
    parents = first_box + jnp.arange(box_a, dtype=jnp.int32)
    child_ids = 2 * parents[:, None] + jnp.arange(2, dtype=jnp.int32)[None, :]
    return parent_level(paired, child_ids, tree_level)


def reference(src_pos, strengths, tgt_pos):
    block_count = src_pos.shape[0]
    group_boxes = src_pos.shape[1] // PER_BOX
    tree_depth = group_boxes.bit_length() - 1
    group_cells = group_boxes * BOX_CELLS
    root_list = []
    for source_blk in range(block_count):
        in_box = (src_pos[source_blk] % BOX_CELLS).reshape(group_boxes, PER_BOX)
        amounts = strengths[:, source_blk].reshape(2, group_boxes, PER_BOX)
        weights = leaf_weights(in_box, amounts)
        for tree_level in range(tree_depth):
            weights = tree_up(weights, tree_level, 0)
        root_list.append(weights.reshape(2, R, group_boxes))
    root_sets = jnp.stack(root_list)
    top_nodes = jnp.asarray(node_offsets(group_cells), jnp.int32)
    final_ticks = TOP_TICKS // group_boxes
    target_count = tgt_pos.shape[0]
    block_size = min(target_count, 65536)

    def one_block(block_no):
        ticks_blk = lax.dynamic_slice_in_dim(tgt_pos, block_no * block_size, block_size, 0)
        box_ids = ticks_blk // final_ticks
        picked = jnp.take(root_sets, box_ids, axis=3)
        angles = turn_angle(ticks_blk[None, :], top_nodes[:, None])
        phase_re = jnp.cos(angles)
        phase_im = jnp.sin(angles)
        field_re = jnp.zeros(ticks_blk.shape, jnp.float32)
        field_imaginary = jnp.zeros(ticks_blk.shape, jnp.float32)
        for source_blk in range(block_count):
            part_re = picked[source_blk, 0]
            part_im = picked[source_blk, 1]
            inner_re = jnp.sum(phase_re * part_re - phase_im * part_im, axis=0)
            inner_im = jnp.sum(phase_re * part_im + phase_im * part_re, axis=0)
            outer_turn = turn_angle(ticks_blk, jnp.int32(source_blk * group_cells))
            outer_re = jnp.cos(outer_turn)
            outer_im = jnp.sin(outer_turn)
            field_re = field_re + outer_re * inner_re - outer_im * inner_im
            field_imaginary = field_imaginary + outer_re * inner_im + outer_im * inner_re
        return jnp.stack([field_re, field_imaginary])

    blocks = lax.map(one_block, jnp.arange(target_count // block_size, dtype=jnp.int32))
    return jnp.transpose(blocks, (1, 0, 2)).reshape(2, target_count)
```

```python
import functools
import math

import jax
import jax.numpy as jnp
import numpy as np
from jax import lax
from jax.experimental import pallas as pl
from jax.experimental.pallas import tpu as pltpu
from jax.sharding import PartitionSpec as P

R = 16
PER_BOX = 128
TGT_BOX = 128
BOX_CELLS = 128
TOP_TICKS = 201326592
LANES = 128
HIGHEST = lax.Precision.HIGHEST


def fit_even(values, span, count):
    u = 0.5 * span * span * (1.0 + np.cos(np.pi * (np.arange(400) + 0.5) / 400))
    cheb = np.polynomial.chebyshev.Chebyshev.fit(u, values(np.sqrt(u)), count - 1, domain=[0, span * span])
    return [float(c) for c in cheb.convert(kind=np.polynomial.Polynomial).coef]


COS_POLY = fit_even(lambda y: np.cos(2 * np.pi * y), 0.5, 6)
SIN_POLY = fit_even(lambda y: np.sin(2 * np.pi * y) / y, 0.5, 6)


def horner(coefs, u):
    out = u * coefs[-1] + coefs[-2]
    for c in coefs[-3::-1]:
        out = out * u + c
    return out


def cos_sin_turns(y):
    u = y * y
    return horner(COS_POLY, u), y * horner(SIN_POLY, u)


def node_offsets(box_cells):
    node_index = np.arange(R)
    unit_nodes = (1.0 - np.cos(np.pi * (node_index + 0.5) / R)) / 2.0
    return np.floor(box_cells * unit_nodes).astype(np.int64)


def lagrange_values(node_pos, points):
    rows = []
    for row_node in range(node_pos.shape[0]):
        column = np.ones(points.shape[0])
        for other in range(node_pos.shape[0]):
            if other != row_node:
                column = column * (points - node_pos[other]) / (node_pos[row_node] - node_pos[other])
        rows.append(column)
    return np.stack(rows)


def as_real(m):
    return np.block([[m.real, -m.imag], [m.imag, m.real]])


def turn64(a, b):
    product = (a * b + 2**31) % 2**32 - 2**31
    return product * (2.0 * np.pi / 2.0**32)


@functools.cache
def step_matrix(level):
    cells = BOX_CELLS * 2**level
    child, parent = node_offsets(cells), node_offsets(2 * cells)
    inner = np.concatenate([child, child + cells])
    blend = lagrange_values(parent / (2.0 * cells), inner / (2.0 * cells)).reshape(R, 2, R)
    half = TOP_TICKS // 2 ** (level + 2)
    assert half * cells % 2**32 == 2**31
    out = np.zeros((2, 2, 2 * R, 2 * R))
    for e in range(2):
        phase = np.exp(1j * turn64(half if e else -half, child))
        for j in range(2):
            out[e, j] = as_real((-1.0) ** j * blend[:, j, :] * phase[None, :])
    return out


def radix_matrix(first, count):
    total = np.eye(2 * R)[None, None]
    for k in range(count):
        m = step_matrix(first + k)
        n = total.shape[0]
        new = np.zeros((2 * n, 2 * n, 2 * R, 2 * R))
        for a in range(n):
            for b in range(n):
                for e in range(2):
                    for j in range(2):
                        new[2 * a + e, b + j * n] = m[e, j] @ total[a, b]
        total = new
    n = total.shape[0]
    return total.transpose(0, 2, 1, 3).reshape(n * 2 * R, n * 2 * R)


def fold_pairs():
    eye = np.eye(R)
    plus = eye[: R // 2] + eye[::-1][: R // 2]
    minus = eye[: R // 2] - eye[::-1][: R // 2]
    zero = np.zeros_like(plus)
    return np.block([[plus, zero], [zero, plus], [zero, -minus], [minus, zero]])


def leaf_matrix():
    nodes = node_offsets(BOX_CELLS)
    angles = np.pi * (np.arange(R) + 0.5) / R
    at_exact = lagrange_values(2.0 * nodes / BOX_CELLS - 1.0, np.cos(angles))
    cheb_at = np.stack([np.cos(n * angles) for n in range(R)])
    norm = np.where(np.arange(R) == 0, 1.0, 2.0) / R
    g = (norm[:, None] * (cheb_at @ at_exact.T)).astype(np.float32)
    wide = np.repeat(g.T, 8, axis=1)
    zero = np.zeros_like(wide)
    return np.block([[wide, zero], [zero, wide]]).astype(np.float32)


def leaf_kernel(pos_ref, str_ref, mix_ref, out_ref, p_t, re_t, im_t, *, digits):
    beta = pl.program_id(0)
    rows = pl.ds(beta, LANES, stride=digits)
    p_t[...] = pos_ref[rows, :].T
    re_t[...] = str_ref[0, rows, :].T
    im_t[...] = str_ref[1, rows, :].T

    def chunk(i, acc):
        here = pl.ds(pl.multiple_of(i * 8, 8), 8)
        r = p_t[here, :] & (BOX_CELLS - 1)
        turn = (r * (TOP_TICKS // 2)).astype(jnp.float32) * (2.0**-32)
        c, s = cos_sin_turns(turn)
        a, b = re_t[here, :], im_t[here, :]
        v = r.astype(jnp.float32) * (2.0 / BOX_CELLS) - 1.0
        v2 = v + v
        re0, im0 = c * a - s * b, s * a + c * b
        re1, im1 = v * re0, v * im0
        new = [(re0, im0), (re1, im1)]
        for _ in range(2, R):
            re0, re1 = re1, v2 * re1 - re0
            im0, im1 = im1, v2 * im1 - im0
            new.append((re1, im1))
        return tuple((x + u, y + w) for (x, y), (u, w) in zip(acc, new))

    zero = jnp.zeros((8, LANES), jnp.float32)
    acc = lax.fori_loop(0, PER_BOX // 8, chunk, tuple((zero, zero) for _ in range(R)), unroll=2)
    stack = jnp.concatenate([x for x, _ in acc] + [y for _, y in acc], axis=0)
    out_ref[0] = jnp.dot(mix_ref[...], stack, precision=HIGHEST, preferred_element_type=jnp.float32)


def leaf_call(pos, strengths):
    boxes = pos.shape[0]
    digits = boxes // LANES
    whole = pl.BlockSpec(memory_space=pltpu.VMEM)
    return pl.pallas_call(
        functools.partial(leaf_kernel, digits=digits),
        grid=(digits,),
        out_shape=jax.ShapeDtypeStruct((digits, 2 * R, LANES), jnp.float32),
        in_specs=[whole, whole, whole],
        out_specs=pl.BlockSpec((1, 2 * R, LANES), lambda b: (b, 0, 0)),
        scratch_shapes=[
            pltpu.VMEM((LANES, LANES), jnp.int32),
            pltpu.VMEM((LANES, LANES), jnp.float32),
            pltpu.VMEM((LANES, LANES), jnp.float32),
        ],
        name="leaf",
    )(pos, strengths, jnp.asarray(leaf_matrix()))


def eval_kernel(suffix_ref, tgt_ref, co_ref, out_ref, g_t, re_t, im_t, *, blocks, leaves, depth, rows):
    cells = BOX_CELLS * 2**depth
    ticks = TOP_TICKS // 2**depth
    half = R // 2
    tile = pl.program_id(0)
    lane = lax.broadcasted_iota(jnp.int32, (1, LANES), 1)
    box = (tile * LANES + lane) * leaves + suffix_ref[0]
    center = box * ticks + ticks // 2
    g_t[...] = (tgt_ref[...].T - center).astype(jnp.float32)
    offsets = 2 * node_offsets(cells) - cells + 1

    def turned(g, factor):
        y = g * factor
        if abs(factor) * (ticks // 2) > 0.5:
            y = y - jnp.round(y)
        return cos_sin_turns(y)

    def chunk(i, carry):
        here = pl.ds(pl.multiple_of(i * rows, rows), rows)
        g = g_t[here, :]
        acc = [[None, None] for _ in range(blocks)]
        for t in range(half):
            c, s = turned(g, float(offsets[t]) * 2.0**-33)
            for q in range(blocks):
                for part in range(2):
                    sc = co_ref[q, pl.ds(part * half + t, 1), :]
                    sd = co_ref[q, pl.ds((2 + part) * half + t, 1), :]
                    term = sc * c + sd * s
                    acc[q][part] = term if t == 0 else acc[q][part] + term
        zc, zs = turned(g, float(cells) * 2.0**-32)
        re, im = acc[blocks - 1]
        for q in range(blocks - 2, -1, -1):
            re, im = zc * re - zs * im + acc[q][0], zc * im + zs * re + acc[q][1]
        pc, ps = turned(g, float(cells - 1) * 2.0**-33)
        re_t[here, :] = pc * re - ps * im
        im_t[here, :] = pc * im + ps * re
        return carry

    lax.fori_loop(0, TGT_BOX // rows, chunk, 0)
    out_ref[pl.ds(0, LANES, stride=2), :] = re_t[...].T
    out_ref[pl.ds(1, LANES, stride=2), :] = im_t[...].T


def eval_call(suffix, ticks, coefs, leaves, depth):
    boxes = ticks.shape[0]
    blocks = coefs.shape[0]
    return pl.pallas_call(
        functools.partial(eval_kernel, blocks=blocks, leaves=leaves, depth=depth, rows=16),
        grid=(boxes // LANES,),
        out_shape=jax.ShapeDtypeStruct((2 * boxes, TGT_BOX), jnp.float32),
        in_specs=[
            pl.BlockSpec(memory_space=pltpu.SMEM),
            pl.BlockSpec((LANES, TGT_BOX), lambda i: (i, 0)),
            pl.BlockSpec((blocks, 2 * R, LANES), lambda i: (0, 0, i)),
        ],
        out_specs=pl.BlockSpec((2 * LANES, TGT_BOX), lambda i: (i, 0)),
        scratch_shapes=[pltpu.VMEM((TGT_BOX, LANES), jnp.float32)] * 3,
        name="evaluate",
    )(suffix.reshape(1), ticks, coefs)


def table(m):
    return jnp.asarray(m.astype(np.float32))


def mm(a, b):
    return jnp.dot(a, b, precision=HIGHEST, preferred_element_type=jnp.float32)


def local_tree(leaf, boxes):
    low = leaf.shape[0]
    n1 = low.bit_length() - 1
    rest = boxes.bit_length() - 1 - n1
    n2 = rest - rest // 2
    n3 = rest - n2
    c = 2 * R
    y = mm(table(radix_matrix(0, n1)), leaf.reshape(low * c, -1))
    y = y.reshape(low, c, 2**n3, 2**n2).transpose(3, 1, 0, 2).reshape(2**n2 * c, -1)
    y = mm(table(radix_matrix(n1, n2)), y)
    y = y.reshape(2**n2, c, low, 2**n3).transpose(3, 1, 2, 0).reshape(2**n3 * c, -1)
    y = mm(table(radix_matrix(n1 + n2, n3)), y)
    return y.reshape(2**n3, c, low * 2**n2).transpose(1, 2, 0).reshape(c, boxes)


def local(src_pos, strengths, tgt_pos):
    leaf_count = lax.axis_size("leaf")
    leaf_bits = leaf_count.bit_length() - 1
    leaf_no = lax.axis_index("leaf")
    boxes = src_pos.shape[1] // PER_BOX
    local_depth = boxes.bit_length() - 1
    leaf = leaf_call(src_pos.reshape(boxes, PER_BOX), strengths.reshape(2, boxes, PER_BOX))
    weights = local_tree(leaf, boxes)
    suffix = jnp.int32(0)
    for bit_no in range(leaf_bits):
        side = leaf_no // 2**bit_no % 2
        route = [(k, k ^ (1 << bit_no)) for k in range(leaf_count)]
        partner = lax.ppermute(weights, "leaf", route)
        m = step_matrix(local_depth + bit_no)
        if bit_no == leaf_bits - 1:
            m = np.einsum("xy,ejyz->ejxz", fold_pairs(), m)
        own = jnp.where(side == 0, table(m[0, 0]), table(m[1, 1]))
        other = jnp.where(side == 0, table(m[0, 1]), table(m[1, 0]))
        weights = mm(own, weights) + mm(other, partner)
        suffix = 2 * suffix + side
    half = boxes // 2
    parts = [lax.all_gather(weights[None, :, i * half : (i + 1) * half], "blk", axis=0, tiled=True) for i in range(2)]
    coefs = jnp.concatenate(parts, axis=2)
    out = eval_call(suffix, tgt_pos.reshape(boxes, TGT_BOX), coefs, leaf_count, local_depth + leaf_bits)
    return out.reshape(boxes, 2, TGT_BOX).transpose(1, 0, 2).reshape(2, boxes * TGT_BOX)


def solution(mesh):
    return jax.shard_map(
        local,
        mesh=mesh,
        in_specs=(P("blk", "leaf"), P(None, "blk", "leaf"), P(("leaf", "blk"))),
        out_specs=P(None, ("leaf", "blk")),
        check_vma=False,
    )
```

```python
import functools
import math

import jax
import jax.numpy as jnp
import numpy as np
from jax import lax
from jax.experimental import pallas as pl
from jax.experimental.pallas import tpu as pltpu
from jax.sharding import PartitionSpec as P

R = 16
PER_BOX = 128
TGT_BOX = 128
BOX_CELLS = 128
TOP_TICKS = 201326592
LANES = 128
HIGHEST = lax.Precision.HIGHEST


def fit_even(values, span, count):
    u = 0.5 * span * span * (1.0 + np.cos(np.pi * (np.arange(400) + 0.5) / 400))
    cheb = np.polynomial.chebyshev.Chebyshev.fit(u, values(np.sqrt(u)), count - 1, domain=[0, span * span])
    return [float(c) for c in cheb.convert(kind=np.polynomial.Polynomial).coef]


COS_POLY = fit_even(lambda y: np.cos(2 * np.pi * y), 0.5, 6)
SIN_POLY = fit_even(lambda y: np.sin(2 * np.pi * y) / y, 0.5, 6)


def horner(coefs, u):
    out = u * coefs[-1] + coefs[-2]
    for c in coefs[-3::-1]:
        out = out * u + c
    return out


def cos_sin_turns(y):
    u = y * y
    return horner(COS_POLY, u), y * horner(SIN_POLY, u)


def node_offsets(box_cells):
    node_index = np.arange(R)
    unit_nodes = (1.0 - np.cos(np.pi * (node_index + 0.5) / R)) / 2.0
    return np.floor(box_cells * unit_nodes).astype(np.int64)


def lagrange_values(node_pos, points):
    rows = []
    for row_node in range(node_pos.shape[0]):
        column = np.ones(points.shape[0])
        for other in range(node_pos.shape[0]):
            if other != row_node:
                column = column * (points - node_pos[other]) / (node_pos[row_node] - node_pos[other])
        rows.append(column)
    return np.stack(rows)


def as_real(m):
    return np.block([[m.real, -m.imag], [m.imag, m.real]])


def turn64(a, b):
    product = (a * b + 2**31) % 2**32 - 2**31
    return product * (2.0 * np.pi / 2.0**32)


@functools.cache
def step_matrix(level):
    cells = BOX_CELLS * 2**level
    child, parent = node_offsets(cells), node_offsets(2 * cells)
    inner = np.concatenate([child, child + cells])
    blend = lagrange_values(parent / (2.0 * cells), inner / (2.0 * cells)).reshape(R, 2, R)
    half = TOP_TICKS // 2 ** (level + 2)
    assert half * cells % 2**32 == 2**31
    out = np.zeros((2, 2, 2 * R, 2 * R))
    for e in range(2):
        phase = np.exp(1j * turn64(half if e else -half, child))
        for j in range(2):
            out[e, j] = as_real((-1.0) ** j * blend[:, j, :] * phase[None, :])
    return out


def radix_matrix(first, count):
    total = np.eye(2 * R)[None, None]
    for k in range(count):
        m = step_matrix(first + k)
        n = total.shape[0]
        new = np.zeros((2 * n, 2 * n, 2 * R, 2 * R))
        for a in range(n):
            for b in range(n):
                for e in range(2):
                    for j in range(2):
                        new[2 * a + e, b + j * n] = m[e, j] @ total[a, b]
        total = new
    n = total.shape[0]
    return total.transpose(0, 2, 1, 3).reshape(n * 2 * R, n * 2 * R)


def fold_pairs():
    eye = np.eye(R)
    plus = eye[: R // 2] + eye[::-1][: R // 2]
    minus = eye[: R // 2] - eye[::-1][: R // 2]
    zero = np.zeros_like(plus)
    return np.block([[plus, zero], [zero, plus], [zero, -minus], [minus, zero]])


def leaf_matrix():
    nodes = node_offsets(BOX_CELLS)
    angles = np.pi * (np.arange(R) + 0.5) / R
    at_exact = lagrange_values(2.0 * nodes / BOX_CELLS - 1.0, np.cos(angles))
    cheb_at = np.stack([np.cos(n * angles) for n in range(R)])
    norm = np.where(np.arange(R) == 0, 1.0, 2.0) / R
    g = (norm[:, None] * (cheb_at @ at_exact.T)).astype(np.float32)
    wide = np.repeat(g.T, 8, axis=1)
    zero = np.zeros_like(wide)
    return np.block([[wide, zero], [zero, wide]]).astype(np.float32)


def leaf_kernel(pos_ref, str_ref, mix_ref, out_ref, p_t, re_t, im_t, *, digits):
    def tile(beta, carry):
        rows = pl.ds(beta, LANES, stride=digits)
        p_t[...] = pos_ref[rows, :].T
        re_t[...] = str_ref[0, rows, :].T
        im_t[...] = str_ref[1, rows, :].T
        zero = jnp.zeros((8, LANES), jnp.float32)
        acc = lax.fori_loop(0, PER_BOX // 8, chunk, tuple((zero, zero) for _ in range(R)), unroll=2)
        low, high = list(acc[: R // 2]), list(acc[R // 2 :])
        top = [high[0]]
        for k in range(1, R // 2):
            top.append(tuple(2.0 * h - m for h, m in zip(high[k], low[R // 2 - k])))
        both = low + top
        stack = jnp.concatenate([x for x, _ in both] + [y for _, y in both], axis=0)
        out_ref[beta] = jnp.dot(mix_ref[...], stack, precision=HIGHEST, preferred_element_type=jnp.float32)
        return carry

    def chunk(i, acc):
        here = pl.ds(pl.multiple_of(i * 8, 8), 8)
        r = p_t[here, :] & (BOX_CELLS - 1)
        turn = (r * (TOP_TICKS // 2)).astype(jnp.float32) * (2.0**-32)
        c, s = cos_sin_turns(turn)
        a, b = re_t[here, :], im_t[here, :]
        v = r.astype(jnp.float32) * (2.0 / BOX_CELLS) - 1.0
        v2 = v + v
        cheb = [None, v]
        for k in range(2, R // 2 + 1):
            cheb.append(v2 * v - 1.0 if k == 2 else v2 * cheb[-1] - cheb[-2])
        x, y = c * a - s * b, s * a + c * b
        out = []
        for part, (x, y) in enumerate([(x, y), (cheb[-1] * x, cheb[-1] * y)]):
            for k in range(R // 2):
                u, w = acc[part * (R // 2) + k]
                out.append((u + x, w + y) if k == 0 else (u + cheb[k] * x, w + cheb[k] * y))
        return tuple(out)

    lax.fori_loop(0, digits, tile, 0)


def leaf_call(pos, strengths):
    boxes = pos.shape[0]
    digits = boxes // LANES
    whole = pl.BlockSpec(memory_space=pltpu.VMEM)
    return pl.pallas_call(
        functools.partial(leaf_kernel, digits=digits),
        out_shape=jax.ShapeDtypeStruct((digits, 2 * R, LANES), jnp.float32),
        in_specs=[whole, whole, whole],
        out_specs=whole,
        scratch_shapes=[
            pltpu.VMEM((LANES, LANES), jnp.int32),
            pltpu.VMEM((LANES, LANES), jnp.float32),
            pltpu.VMEM((LANES, LANES), jnp.float32),
        ],
        name="leaf",
    )(pos, strengths, jnp.asarray(leaf_matrix()))


MAGIC = 1.5 * 2.0**23


def finish_kernel(w_ref, tgt_hbm, m_ref, out_hbm, tgt, out, bufs, got, coefs, g_t, re_t, im_t,
                  send, recv, gsend, grecv, tsem, osem, *, leaves, blocks, chunks, depth, rows):
    leaf_no, blk_no = lax.axis_index("leaf"), lax.axis_index("blk")
    bits = leaves.bit_length() - 1
    boxes = w_ref.shape[1]
    width = boxes // chunks
    tiles = width // LANES
    cells = BOX_CELLS * 2**depth
    ticks = TOP_TICKS // 2**depth
    half = R // 2
    sides = [leaf_no // 2**k % 2 for k in range(bits)]
    partners = [leaf_no + (1 - 2 * sides[k]) * 2**k for k in range(bits)]
    suffix = jnp.int32(0)
    for k in range(bits):
        suffix = 2 * suffix + sides[k]
    peers = [lax.rem(blk_no + d, blocks) for d in range(1, blocks)]
    fetch = pltpu.make_async_copy(tgt_hbm, tgt, tsem)
    fetch.start()

    barrier = pltpu.get_barrier_semaphore()
    for k in range(bits):
        pl.semaphore_signal(barrier, inc=1, device_id=(partners[k], blk_no), device_id_type=pl.DeviceIdType.MESH)
    for peer in peers:
        pl.semaphore_signal(barrier, inc=1, device_id=(leaf_no, peer), device_id_type=pl.DeviceIdType.MESH)
    pl.semaphore_wait(barrier, bits + blocks - 1)

    def own(stage, c):
        return w_ref.at[:, pl.ds(c * width, width)] if stage == 0 else bufs.at[stage - 1, c]

    def exchange(stage, c):
        return pltpu.make_async_remote_copy(
            src_ref=own(stage, c), dst_ref=got.at[stage, c],
            send_sem=send.at[stage, c], recv_sem=recv.at[stage, c],
            device_id=(partners[stage], blk_no), device_id_type=pl.DeviceIdType.MESH,
        )

    def spread(d, c):
        here = coefs.at[blk_no, pl.ds(c * tiles, tiles)]
        return pltpu.make_async_remote_copy(
            src_ref=here, dst_ref=here,
            send_sem=gsend.at[d - 1, c], recv_sem=grecv.at[d - 1, c],
            device_id=(leaf_no, peers[d - 1]), device_id_type=pl.DeviceIdType.MESH,
        )

    def combine(stage, c):
        exchange(stage, c).wait_recv()
        m_own, m_other = m_ref[stage, sides[stage], 0], m_ref[stage, sides[stage], 1]
        w = mm(m_own, own(stage, c)[...]) + mm(m_other, got[stage, c])
        if stage < bits - 1:
            bufs[stage, c] = w
            exchange(stage + 1, c).start()
        else:
            for i in range(tiles):
                coefs[blk_no, c * tiles + i] = w[:, i * LANES : (i + 1) * LANES]
            for d in range(1, blocks):
                spread(d, c).start()

    offsets = 2 * node_offsets(cells) - cells + 1

    def turned(g, factor):
        y = g * factor
        if abs(factor) * (ticks // 2) > 0.5:
            y = y - ((y + MAGIC) - MAGIC)
        return cos_sin_turns(y)

    lane = lax.broadcasted_iota(jnp.int32, (1, LANES), 1)

    def evaluate(tile, carry):
        box = (tile * LANES + lane) * leaves + suffix
        center = box * ticks + ticks // 2
        first = pl.multiple_of(tile * LANES, LANES)
        g_t[...] = (tgt[pl.ds(first, LANES), :].T - center).astype(jnp.float32)

        def chunk(i, carry):
            here = pl.ds(pl.multiple_of(i * rows, rows), rows)
            g = g_t[here, :]
            acc = [[None, None] for _ in range(blocks)]
            for t in range(half):
                c, s = turned(g, float(offsets[t]) * 2.0**-33)
                for q in range(blocks):
                    for part in range(2):
                        sc = coefs[q, tile, pl.ds(part * half + t, 1), :]
                        sd = coefs[q, tile, pl.ds((2 + part) * half + t, 1), :]
                        term = sc * c + sd * s
                        acc[q][part] = term if t == 0 else acc[q][part] + term
            zc, zs = turned(g, float(cells) * 2.0**-32)
            re, im = acc[blocks - 1]
            for q in range(blocks - 2, -1, -1):
                re, im = zc * re - zs * im + acc[q][0], zc * im + zs * re + acc[q][1]
            pc, ps = turned(g, float(cells - 1) * 2.0**-33)
            re_t[here, :] = pc * re - ps * im
            im_t[here, :] = pc * im + ps * re
            return carry

        lax.fori_loop(0, TGT_BOX // rows, chunk, 0)
        out[pl.ds(2 * first, LANES, stride=2), :] = re_t[...].T
        out[pl.ds(2 * first + 1, LANES, stride=2), :] = im_t[...].T
        return carry

    def put(c):
        span = pl.ds(2 * c * width, 2 * width)
        return pltpu.make_async_copy(out.at[span], out_hbm.at[span], osem.at[c])

    def field(c):
        if c == 0:
            fetch.wait()
        for d in range(1, blocks):
            spread(d, c).wait_recv()
        lax.fori_loop(c * tiles, (c + 1) * tiles, evaluate, 0)
        put(c).start()

    for c in range(chunks):
        exchange(0, c).start()
    for step in range(chunks + bits - 2):
        for stage in range(bits - 1, -1, -1):
            if 0 <= step - stage < chunks:
                combine(stage, step - stage)
    field(0)
    combine(bits - 1, chunks - 1)
    for c in range(1, chunks):
        field(c)
    for c in range(chunks):
        for stage in range(bits):
            exchange(stage, c).wait_send()
        for d in range(1, blocks):
            spread(d, c).wait_send()
        put(c).wait()


def finish_call(weights, ticks, matrices, leaves, blocks, depth, chunks):
    boxes = ticks.shape[0]
    bits = leaves.bit_length() - 1
    width = boxes // chunks
    whole = pl.BlockSpec(memory_space=pltpu.VMEM)
    anywhere = pl.BlockSpec(memory_space=pl.ANY)
    dma = pltpu.SemaphoreType.DMA
    return pl.pallas_call(
        functools.partial(finish_kernel, leaves=leaves, blocks=blocks, chunks=chunks, depth=depth, rows=16),
        out_shape=jax.ShapeDtypeStruct((2 * boxes, TGT_BOX), jnp.float32),
        in_specs=[whole, anywhere, whole],
        out_specs=anywhere,
        scratch_shapes=[
            pltpu.VMEM((boxes, TGT_BOX), jnp.int32),
            pltpu.VMEM((2 * boxes, TGT_BOX), jnp.float32),
            pltpu.VMEM((bits - 1, chunks, 2 * R, width), jnp.float32),
            pltpu.VMEM((bits, chunks, 2 * R, width), jnp.float32),
            pltpu.VMEM((blocks, boxes // LANES, 2 * R, LANES), jnp.float32),
        ] + [pltpu.VMEM((TGT_BOX, LANES), jnp.float32)] * 3 + [
            dma((bits, chunks)), dma((bits, chunks)),
            dma((blocks - 1, chunks)), dma((blocks - 1, chunks)),
            dma, dma((chunks,)),
        ],
        compiler_params=pltpu.CompilerParams(collective_id=0, has_side_effects=True),
        name="finish",
    )(weights, ticks, matrices)


def table(m):
    return jnp.asarray(m.astype(np.float32))


def mm(a, b):
    return jnp.dot(a, b, precision=HIGHEST, preferred_element_type=jnp.float32)


def local_tree(leaf, boxes):
    low = leaf.shape[0]
    n1 = low.bit_length() - 1
    rest = boxes.bit_length() - 1 - n1
    n2 = rest - rest // 2
    n3 = rest - n2
    c = 2 * R
    y = mm(table(radix_matrix(0, n1)), leaf.reshape(low * c, -1))
    y = y.reshape(low, c, 2**n3, 2**n2).transpose(3, 1, 0, 2).reshape(2**n2 * c, -1)
    y = mm(table(radix_matrix(n1, n2)), y)
    y = y.reshape(2**n2, c, low, 2**n3).transpose(3, 1, 2, 0).reshape(2**n3 * c, -1)
    y = mm(table(radix_matrix(n1 + n2, n3)), y)
    return y.reshape(2**n3, c, low * 2**n2).transpose(1, 2, 0).reshape(c, boxes)


def local(src_pos, strengths, tgt_pos):
    leaf_count = lax.axis_size("leaf")
    leaf_bits = leaf_count.bit_length() - 1
    boxes = src_pos.shape[1] // PER_BOX
    local_depth = boxes.bit_length() - 1
    leaf = leaf_call(src_pos.reshape(boxes, PER_BOX), strengths.reshape(2, boxes, PER_BOX))
    weights = local_tree(leaf, boxes)
    steps = np.stack([step_matrix(local_depth + k) for k in range(leaf_bits)])
    steps[-1] = np.einsum("xy,ejyz->ejxz", fold_pairs(), steps[-1])
    steps[:, 1] = steps[:, 1, ::-1]
    out = finish_call(
        weights, tgt_pos.reshape(boxes, TGT_BOX), table(steps), leaf_count, lax.axis_size("blk"),
        local_depth + leaf_bits, 4,
    )
    return out.reshape(boxes, 2, TGT_BOX).transpose(1, 0, 2).reshape(2, boxes * TGT_BOX)


def solution(mesh):
    return jax.shard_map(
        local,
        mesh=mesh,
        in_specs=(P("blk", "leaf"), P(None, "blk", "leaf"), P(("leaf", "blk"))),
        out_specs=P(None, ("leaf", "blk")),
        check_vma=False,
    )
```

```python
import functools
import math

import jax
import jax.numpy as jnp
import numpy as np
from jax import lax
from jax.experimental import pallas as pl
from jax.experimental.pallas import tpu as pltpu
from jax.sharding import PartitionSpec as P

R = 16
PER_BOX = 128
TGT_BOX = 128
BOX_CELLS = 128
TOP_TICKS = 201326592
LANES = 128
HIGHEST = lax.Precision.HIGHEST


def fit_even(values, span, count):
    u = 0.5 * span * span * (1.0 + np.cos(np.pi * (np.arange(400) + 0.5) / 400))
    cheb = np.polynomial.chebyshev.Chebyshev.fit(u, values(np.sqrt(u)), count - 1, domain=[0, span * span])
    return [float(c) for c in cheb.convert(kind=np.polynomial.Polynomial).coef]


COS_POLY = fit_even(lambda y: np.cos(np.pi * y), 0.5, 5)
SIN_POLY = fit_even(lambda y: np.sin(np.pi * y) / y, 0.5, 4)


def horner(coefs, u):
    out = u * coefs[-1] + coefs[-2]
    for c in coefs[-3::-1]:
        out = out * u + c
    return out


def cos_sin_turns(y):
    u = y * y
    c, s = horner(COS_POLY, u), y * horner(SIN_POLY, u)
    twice = s + s
    return 1.0 - twice * s, twice * c


def node_offsets(box_cells):
    node_index = np.arange(R)
    unit_nodes = (1.0 - np.cos(np.pi * (node_index + 0.5) / R)) / 2.0
    return np.floor(box_cells * unit_nodes).astype(np.int64)


def lagrange_values(node_pos, points):
    rows = []
    for row_node in range(node_pos.shape[0]):
        column = np.ones(points.shape[0])
        for other in range(node_pos.shape[0]):
            if other != row_node:
                column = column * (points - node_pos[other]) / (node_pos[row_node] - node_pos[other])
        rows.append(column)
    return np.stack(rows)


def as_real(m):
    return np.block([[m.real, -m.imag], [m.imag, m.real]])


def turn64(a, b):
    product = (a * b + 2**31) % 2**32 - 2**31
    return product * (2.0 * np.pi / 2.0**32)


@functools.cache
def step_matrix(level):
    cells = BOX_CELLS * 2**level
    child, parent = node_offsets(cells), node_offsets(2 * cells)
    inner = np.concatenate([child, child + cells])
    blend = lagrange_values(parent / (2.0 * cells), inner / (2.0 * cells)).reshape(R, 2, R)
    half = TOP_TICKS // 2 ** (level + 2)
    assert half * cells % 2**32 == 2**31
    out = np.zeros((2, 2, 2 * R, 2 * R))
    for e in range(2):
        phase = np.exp(1j * turn64(half if e else -half, child))
        for j in range(2):
            out[e, j] = as_real((-1.0) ** j * blend[:, j, :] * phase[None, :])
    return out


def radix_matrix(first, count):
    total = np.eye(2 * R)[None, None]
    for k in range(count):
        m = step_matrix(first + k)
        n = total.shape[0]
        new = np.zeros((2 * n, 2 * n, 2 * R, 2 * R))
        for a in range(n):
            for b in range(n):
                for e in range(2):
                    for j in range(2):
                        new[2 * a + e, b + j * n] = m[e, j] @ total[a, b]
        total = new
    n = total.shape[0]
    return total.transpose(0, 2, 1, 3).reshape(n * 2 * R, n * 2 * R)


def fold_pairs():
    eye = np.eye(R)
    plus = eye[: R // 2] + eye[::-1][: R // 2]
    minus = eye[: R // 2] - eye[::-1][: R // 2]
    zero = np.zeros_like(plus)
    return np.block([[plus, zero], [zero, plus], [zero, -minus], [minus, zero]])


def leaf_matrix():
    nodes = node_offsets(BOX_CELLS)
    angles = np.pi * (np.arange(R) + 0.5) / R
    at_exact = lagrange_values(2.0 * nodes / BOX_CELLS - 1.0, np.cos(angles))
    cheb_at = np.stack([np.cos(n * angles) for n in range(R)])
    norm = np.where(np.arange(R) == 0, 1.0, 2.0) / R
    g = (norm[:, None] * (cheb_at @ at_exact.T)).astype(np.float32)
    wide = np.repeat(g.T, 8, axis=1)
    zero = np.zeros_like(wide)
    return np.block([[wide, zero], [zero, wide]]).astype(np.float32)


def leaf_kernel(pos_ref, str_ref, mix_ref, out_ref, p_t, re_t, im_t, *, digits):
    def turn_over(beta, slot):
        rows = pl.ds(beta, LANES, stride=digits)
        p_t[slot] = pos_ref[rows, :].T
        re_t[slot] = str_ref[0, rows, :].T
        im_t[slot] = str_ref[1, rows, :].T

    def tile(beta, carry):
        slot = lax.rem(beta, 2)
        turn_over(jnp.minimum(beta + 1, digits - 1), 1 - slot)
        zero = jnp.zeros((8, LANES), jnp.float32)
        acc = tuple((zero, zero) for _ in range(R))
        for i in range(PER_BOX // 8):
            acc = chunk(slot, i, acc)
        low, high = list(acc[: R // 2]), list(acc[R // 2 :])
        top = [high[0]]
        for k in range(1, R // 2):
            top.append(tuple(2.0 * h - m for h, m in zip(high[k], low[R // 2 - k])))
        both = low + top
        stack = jnp.concatenate([x for x, _ in both] + [y for _, y in both], axis=0)
        out_ref[beta] = jnp.dot(mix_ref[...], stack, precision=HIGHEST, preferred_element_type=jnp.float32)
        return carry

    def chunk(slot, i, acc):
        here = pl.ds(i * 8, 8)
        r = p_t[slot, here, :] & (BOX_CELLS - 1)
        turn = (r * (TOP_TICKS // 2)).astype(jnp.float32) * (2.0**-32)
        c, s = cos_sin_turns(turn)
        a, b = re_t[slot, here, :], im_t[slot, here, :]
        v = r.astype(jnp.float32) * (2.0 / BOX_CELLS) - 1.0
        v2 = v + v
        cheb = [None, v]
        for k in range(2, R // 2 + 1):
            cheb.append(v2 * v - 1.0 if k == 2 else v2 * cheb[-1] - cheb[-2])
        x, y = c * a - s * b, s * a + c * b
        out = []
        for part, (x, y) in enumerate([(x, y), (cheb[-1] * x, cheb[-1] * y)]):
            for k in range(R // 2):
                u, w = acc[part * (R // 2) + k]
                out.append((u + x, w + y) if k == 0 else (u + cheb[k] * x, w + cheb[k] * y))
        return tuple(out)

    turn_over(0, 0)
    lax.fori_loop(0, digits, tile, 0)


def leaf_call(pos, strengths):
    boxes = pos.shape[0]
    digits = boxes // LANES
    whole = pl.BlockSpec(memory_space=pltpu.VMEM)
    return pl.pallas_call(
        functools.partial(leaf_kernel, digits=digits),
        out_shape=jax.ShapeDtypeStruct((digits, 2 * R, LANES), jnp.float32),
        in_specs=[whole, whole, whole],
        out_specs=whole,
        scratch_shapes=[
            pltpu.VMEM((2, LANES, LANES), jnp.int32),
            pltpu.VMEM((2, LANES, LANES), jnp.float32),
            pltpu.VMEM((2, LANES, LANES), jnp.float32),
        ],
        name="leaf",
    )(pos, strengths, jnp.asarray(leaf_matrix()))


MAGIC = 1.5 * 2.0**23


def finish_kernel(w_ref, tgt_hbm, m_ref, out_hbm, tgt, out, bufs, got, coefs, g_t, re_t, im_t,
                  send, recv, gsend, grecv, tsem, osem, *, leaves, blocks, chunks, depth, rows):
    leaf_no, blk_no = lax.axis_index("leaf"), lax.axis_index("blk")
    bits = leaves.bit_length() - 1
    boxes = w_ref.shape[1]
    width = boxes // chunks
    tiles = width // LANES
    cells = BOX_CELLS * 2**depth
    ticks = TOP_TICKS // 2**depth
    half = R // 2
    sides = [leaf_no // 2**k % 2 for k in range(bits)]
    partners = [leaf_no + (1 - 2 * sides[k]) * 2**k for k in range(bits)]
    suffix = jnp.int32(0)
    for k in range(bits):
        suffix = 2 * suffix + sides[k]
    peers = [lax.rem(blk_no + d, blocks) for d in range(1, blocks)]
    fetch = pltpu.make_async_copy(tgt_hbm, tgt, tsem)
    fetch.start()

    barrier = pltpu.get_barrier_semaphore()
    for k in range(bits):
        pl.semaphore_signal(barrier, inc=1, device_id=(partners[k], blk_no), device_id_type=pl.DeviceIdType.MESH)
    for peer in peers:
        pl.semaphore_signal(barrier, inc=1, device_id=(leaf_no, peer), device_id_type=pl.DeviceIdType.MESH)
    pl.semaphore_wait(barrier, bits + blocks - 1)

    def own(stage, c):
        return w_ref.at[:, pl.ds(c * width, width)] if stage == 0 else bufs.at[stage - 1, c]

    def exchange(stage, c):
        return pltpu.make_async_remote_copy(
            src_ref=own(stage, c), dst_ref=got.at[stage, c],
            send_sem=send.at[stage, c], recv_sem=recv.at[stage, c],
            device_id=(partners[stage], blk_no), device_id_type=pl.DeviceIdType.MESH,
        )

    def spread(d, c):
        here = coefs.at[blk_no, pl.ds(c * tiles, tiles)]
        return pltpu.make_async_remote_copy(
            src_ref=here, dst_ref=here,
            send_sem=gsend.at[d - 1, c], recv_sem=grecv.at[d - 1, c],
            device_id=(leaf_no, peers[d - 1]), device_id_type=pl.DeviceIdType.MESH,
        )

    def combine(stage, c):
        exchange(stage, c).wait_recv()
        m_own, m_other = m_ref[stage, sides[stage], 0], m_ref[stage, sides[stage], 1]
        w = mm(m_own, own(stage, c)[...]) + mm(m_other, got[stage, c])
        if stage < bits - 1:
            bufs[stage, c] = w
            exchange(stage + 1, c).start()
        else:
            for i in range(tiles):
                coefs[blk_no, c * tiles + i] = w[:, i * LANES : (i + 1) * LANES]
            for d in range(1, blocks):
                spread(d, c).start()

    offsets = 2 * node_offsets(cells) - cells + 1

    def turned(g, factor):
        y = g * factor
        if abs(factor) * (ticks // 2) > 0.5:
            y = y - ((y + MAGIC) - MAGIC)
        return cos_sin_turns(y)

    lane = lax.broadcasted_iota(jnp.int32, (1, LANES), 1)

    def evaluate(tile, carry):
        box = (tile * LANES + lane) * leaves + suffix
        center = box * ticks + ticks // 2
        first = pl.multiple_of(tile * LANES, LANES)
        g_t[...] = (tgt[pl.ds(first, LANES), :].T - center).astype(jnp.float32)

        def chunk(i, carry):
            here = pl.ds(pl.multiple_of(i * rows, rows), rows)
            g = g_t[here, :]
            acc = [[None, None] for _ in range(blocks)]
            for t in range(half):
                c, s = turned(g, float(offsets[t]) * 2.0**-33)
                for q in range(blocks):
                    for part in range(2):
                        sc = coefs[q, tile, pl.ds(part * half + t, 1), :]
                        sd = coefs[q, tile, pl.ds((2 + part) * half + t, 1), :]
                        term = sc * c + sd * s
                        acc[q][part] = term if t == 0 else acc[q][part] + term
            zc, zs = turned(g, float(cells) * 2.0**-32)
            re, im = acc[blocks - 1]
            for q in range(blocks - 2, -1, -1):
                re, im = zc * re - zs * im + acc[q][0], zc * im + zs * re + acc[q][1]
            pc, ps = turned(g, float(cells - 1) * 2.0**-33)
            re_t[here, :] = pc * re - ps * im
            im_t[here, :] = pc * im + ps * re
            return carry

        lax.fori_loop(0, TGT_BOX // rows, chunk, 0)
        out[pl.ds(2 * first, LANES, stride=2), :] = re_t[...].T
        out[pl.ds(2 * first + 1, LANES, stride=2), :] = im_t[...].T
        return carry

    def put(c):
        span = pl.ds(2 * c * width, 2 * width)
        return pltpu.make_async_copy(out.at[span], out_hbm.at[span], osem.at[c])

    def field(c):
        if c == 0:
            fetch.wait()
        for d in range(1, blocks):
            spread(d, c).wait_recv()
        lax.fori_loop(c * tiles, (c + 1) * tiles, evaluate, 0)
        put(c).start()

    ahead = min(3, chunks)
    for c in range(ahead):
        exchange(0, c).start()
    for step in range(chunks + bits):
        for stage in range(bits - 1, -1, -1):
            if 0 <= step - stage < chunks:
                combine(stage, step - stage)
        if step + ahead < chunks:
            exchange(0, step + ahead).start()
        if step >= bits:
            field(step - bits)
    for c in range(chunks):
        for stage in range(bits):
            exchange(stage, c).wait_send()
        for d in range(1, blocks):
            spread(d, c).wait_send()
        put(c).wait()


def finish_call(weights, ticks, matrices, leaves, blocks, depth, chunks):
    boxes = ticks.shape[0]
    bits = leaves.bit_length() - 1
    width = boxes // chunks
    whole = pl.BlockSpec(memory_space=pltpu.VMEM)
    anywhere = pl.BlockSpec(memory_space=pl.ANY)
    dma = pltpu.SemaphoreType.DMA
    return pl.pallas_call(
        functools.partial(finish_kernel, leaves=leaves, blocks=blocks, chunks=chunks, depth=depth, rows=16),
        out_shape=jax.ShapeDtypeStruct((2 * boxes, TGT_BOX), jnp.float32),
        in_specs=[whole, anywhere, whole],
        out_specs=anywhere,
        scratch_shapes=[
            pltpu.VMEM((boxes, TGT_BOX), jnp.int32),
            pltpu.VMEM((2 * boxes, TGT_BOX), jnp.float32),
            pltpu.VMEM((bits - 1, chunks, 2 * R, width), jnp.float32),
            pltpu.VMEM((bits, chunks, 2 * R, width), jnp.float32),
            pltpu.VMEM((blocks, boxes // LANES, 2 * R, LANES), jnp.float32),
        ] + [pltpu.VMEM((TGT_BOX, LANES), jnp.float32)] * 3 + [
            dma((bits, chunks)), dma((bits, chunks)),
            dma((blocks - 1, chunks)), dma((blocks - 1, chunks)),
            dma, dma((chunks,)),
        ],
        compiler_params=pltpu.CompilerParams(collective_id=0, has_side_effects=True),
        name="finish",
    )(weights, ticks, matrices)


def table(m):
    return jnp.asarray(m.astype(np.float32))


def mm(a, b):
    return jnp.dot(a, b, precision=HIGHEST, preferred_element_type=jnp.float32)


def local_tree(leaf, boxes):
    low = leaf.shape[0]
    n1 = low.bit_length() - 1
    rest = boxes.bit_length() - 1 - n1
    n2 = rest - rest // 2
    n3 = rest - n2
    c = 2 * R
    y = mm(table(radix_matrix(0, n1)), leaf.reshape(low * c, -1))
    y = y.reshape(low, c, 2**n3, 2**n2).transpose(3, 1, 0, 2).reshape(2**n2 * c, -1)
    y = mm(table(radix_matrix(n1, n2)), y)
    y = y.reshape(2**n2, c, low, 2**n3).transpose(3, 1, 2, 0).reshape(2**n3 * c, -1)
    y = mm(table(radix_matrix(n1 + n2, n3)), y)
    return y.reshape(2**n3, c, low * 2**n2).transpose(1, 2, 0).reshape(c, boxes)


def local(src_pos, strengths, tgt_pos):
    leaf_count = lax.axis_size("leaf")
    leaf_bits = leaf_count.bit_length() - 1
    boxes = src_pos.shape[1] // PER_BOX
    local_depth = boxes.bit_length() - 1
    leaf = leaf_call(src_pos.reshape(boxes, PER_BOX), strengths.reshape(2, boxes, PER_BOX))
    weights = local_tree(leaf, boxes)
    steps = np.stack([step_matrix(local_depth + k) for k in range(leaf_bits)])
    steps[-1] = np.einsum("xy,ejyz->ejxz", fold_pairs(), steps[-1])
    steps[:, 1] = steps[:, 1, ::-1]
    out = finish_call(
        weights, tgt_pos.reshape(boxes, TGT_BOX), table(steps), leaf_count, lax.axis_size("blk"),
        local_depth + leaf_bits, 8,
    )
    return out.reshape(boxes, 2, TGT_BOX).transpose(1, 0, 2).reshape(2, boxes * TGT_BOX)


def solution(mesh):
    return jax.shard_map(
        local,
        mesh=mesh,
        in_specs=(P("blk", "leaf"), P(None, "blk", "leaf"), P(("leaf", "blk"))),
        out_specs=P(None, ("leaf", "blk")),
        check_vma=False,
    )
```

```python
import functools
import math

import jax
import jax.numpy as jnp
import numpy as np
from jax import lax
from jax.experimental import pallas as pl
from jax.experimental.pallas import tpu as pltpu
from jax.sharding import PartitionSpec as P

R = 16
PER_BOX = 128
TGT_BOX = 128
BOX_CELLS = 128
TOP_TICKS = 201326592
LANES = 128
HIGHEST = lax.Precision.HIGHEST


def fit_even(values, span, count):
    u = 0.5 * span * span * (1.0 + np.cos(np.pi * (np.arange(400) + 0.5) / 400))
    cheb = np.polynomial.chebyshev.Chebyshev.fit(u, values(np.sqrt(u)), count - 1, domain=[0, span * span])
    return [float(c) for c in cheb.convert(kind=np.polynomial.Polynomial).coef]


COS_POLY = fit_even(lambda y: np.cos(np.pi * y), 0.5, 5)
SIN_POLY = fit_even(lambda y: np.sin(np.pi * y) / y, 0.5, 4)


def horner(coefs, u):
    out = u * coefs[-1] + coefs[-2]
    for c in coefs[-3::-1]:
        out = out * u + c
    return out


def cos_sin_turns(y):
    u = y * y
    c, s = horner(COS_POLY, u), y * horner(SIN_POLY, u)
    twice = s + s
    return 1.0 - twice * s, twice * c


def node_offsets(box_cells):
    node_index = np.arange(R)
    unit_nodes = (1.0 - np.cos(np.pi * (node_index + 0.5) / R)) / 2.0
    return np.floor(box_cells * unit_nodes).astype(np.int64)


def lagrange_values(node_pos, points):
    rows = []
    for row_node in range(node_pos.shape[0]):
        column = np.ones(points.shape[0])
        for other in range(node_pos.shape[0]):
            if other != row_node:
                column = column * (points - node_pos[other]) / (node_pos[row_node] - node_pos[other])
        rows.append(column)
    return np.stack(rows)


def as_real(m):
    return np.block([[m.real, -m.imag], [m.imag, m.real]])


def turn64(a, b):
    product = (a * b + 2**31) % 2**32 - 2**31
    return product * (2.0 * np.pi / 2.0**32)


@functools.cache
def step_matrix(level):
    cells = BOX_CELLS * 2**level
    child, parent = node_offsets(cells), node_offsets(2 * cells)
    inner = np.concatenate([child, child + cells])
    blend = lagrange_values(parent / (2.0 * cells), inner / (2.0 * cells)).reshape(R, 2, R)
    half = TOP_TICKS // 2 ** (level + 2)
    assert half * cells % 2**32 == 2**31
    out = np.zeros((2, 2, 2 * R, 2 * R))
    for e in range(2):
        phase = np.exp(1j * turn64(half if e else -half, child))
        for j in range(2):
            out[e, j] = as_real((-1.0) ** j * blend[:, j, :] * phase[None, :])
    return out


def radix_matrix(first, count):
    total = np.eye(2 * R)[None, None]
    for k in range(count):
        m = step_matrix(first + k)
        n = total.shape[0]
        new = np.zeros((2 * n, 2 * n, 2 * R, 2 * R))
        for a in range(n):
            for b in range(n):
                for e in range(2):
                    for j in range(2):
                        new[2 * a + e, b + j * n] = m[e, j] @ total[a, b]
        total = new
    n = total.shape[0]
    return total.transpose(0, 2, 1, 3).reshape(n * 2 * R, n * 2 * R)


def fold_pairs():
    eye = np.eye(R)
    plus = eye[: R // 2] + eye[::-1][: R // 2]
    minus = eye[: R // 2] - eye[::-1][: R // 2]
    zero = np.zeros_like(plus)
    return np.block([[plus, zero], [zero, plus], [zero, -minus], [minus, zero]])


def leaf_matrix():
    nodes = node_offsets(BOX_CELLS)
    angles = np.pi * (np.arange(R) + 0.5) / R
    at_exact = lagrange_values(2.0 * nodes / BOX_CELLS - 1.0, np.cos(angles))
    cheb_at = np.stack([np.cos(n * angles) for n in range(R)])
    norm = np.where(np.arange(R) == 0, 1.0, 2.0) / R
    g = (norm[:, None] * (cheb_at @ at_exact.T)).astype(np.float32)
    wide = np.repeat(g.T, 8, axis=1)
    zero = np.zeros_like(wide)
    return np.block([[wide, zero], [zero, wide]]).astype(np.float32)


def leaf_kernel(pos_ref, str_ref, mix_ref, out_ref, p_t, re_t, im_t, *, digits):
    def turn_over(beta, slot):
        rows = pl.ds(beta, LANES, stride=digits)
        p_t[slot] = pos_ref[rows, :].T
        re_t[slot] = str_ref[0, rows, :].T
        im_t[slot] = str_ref[1, rows, :].T

    def tile(beta, carry):
        slot = lax.rem(beta, 2)
        turn_over(jnp.minimum(beta + 1, digits - 1), 1 - slot)
        zero = jnp.zeros((8, LANES), jnp.float32)
        acc = tuple((zero, zero) for _ in range(R))
        for i in range(PER_BOX // 8):
            acc = chunk(slot, i, acc)
        low, high = list(acc[: R // 2]), list(acc[R // 2 :])
        top = [high[0]]
        for k in range(1, R // 2):
            top.append(tuple(2.0 * h - m for h, m in zip(high[k], low[R // 2 - k])))
        both = low + top
        stack = jnp.concatenate([x for x, _ in both] + [y for _, y in both], axis=0)
        out_ref[beta] = jnp.dot(mix_ref[...], stack, precision=HIGHEST, preferred_element_type=jnp.float32)
        return carry

    def chunk(slot, i, acc):
        here = pl.ds(i * 8, 8)
        r = p_t[slot, here, :] & (BOX_CELLS - 1)
        turn = (r * (TOP_TICKS // 2)).astype(jnp.float32) * (2.0**-32)
        c, s = cos_sin_turns(turn)
        a, b = re_t[slot, here, :], im_t[slot, here, :]
        v = r.astype(jnp.float32) * (2.0 / BOX_CELLS) - 1.0
        v2 = v + v
        cheb = [None, v]
        for k in range(2, R // 2 + 1):
            cheb.append(v2 * v - 1.0 if k == 2 else v2 * cheb[-1] - cheb[-2])
        x, y = c * a - s * b, s * a + c * b
        out = []
        for part, (x, y) in enumerate([(x, y), (cheb[-1] * x, cheb[-1] * y)]):
            for k in range(R // 2):
                u, w = acc[part * (R // 2) + k]
                out.append((u + x, w + y) if k == 0 else (u + cheb[k] * x, w + cheb[k] * y))
        return tuple(out)

    turn_over(0, 0)
    lax.fori_loop(0, digits, tile, 0)


def leaf_call(pos, strengths):
    boxes = pos.shape[0]
    digits = boxes // LANES
    whole = pl.BlockSpec(memory_space=pltpu.VMEM)
    return pl.pallas_call(
        functools.partial(leaf_kernel, digits=digits),
        out_shape=jax.ShapeDtypeStruct((digits, 2 * R, LANES), jnp.float32),
        in_specs=[whole, whole, whole],
        out_specs=whole,
        scratch_shapes=[
            pltpu.VMEM((2, LANES, LANES), jnp.int32),
            pltpu.VMEM((2, LANES, LANES), jnp.float32),
            pltpu.VMEM((2, LANES, LANES), jnp.float32),
        ],
        name="leaf",
    )(pos, strengths, jnp.asarray(leaf_matrix()))


MAGIC = 1.5 * 2.0**23


def finish_kernel(w_ref, tgt_hbm, m_ref, out_hbm, tgt, out, bufs, got, coefs, g_t, re_t, im_t,
                  send, recv, gsend, grecv, tsem, osem, *, leaves, blocks, chunks, depth, rows):
    leaf_no, blk_no = lax.axis_index("leaf"), lax.axis_index("blk")
    bits = leaves.bit_length() - 1
    boxes = w_ref.shape[1]
    width = boxes // chunks
    tiles = width // LANES
    cells = BOX_CELLS * 2**depth
    ticks = TOP_TICKS // 2**depth
    half = R // 2
    sides = [leaf_no // 2**k % 2 for k in range(bits)]
    partners = [leaf_no + (1 - 2 * sides[k]) * 2**k for k in range(bits)]
    suffix = jnp.int32(0)
    for k in range(bits):
        suffix = 2 * suffix + sides[k]
    peers = [lax.rem(blk_no + d, blocks) for d in range(1, blocks)]
    fetch = pltpu.make_async_copy(tgt_hbm, tgt, tsem)
    fetch.start()

    barrier = pltpu.get_barrier_semaphore()
    for k in range(bits):
        pl.semaphore_signal(barrier, inc=1, device_id=(partners[k], blk_no), device_id_type=pl.DeviceIdType.MESH)
    for peer in peers:
        pl.semaphore_signal(barrier, inc=1, device_id=(leaf_no, peer), device_id_type=pl.DeviceIdType.MESH)
    pl.semaphore_wait(barrier, bits + blocks - 1)

    def own(stage, c):
        return w_ref.at[:, pl.ds(c * width, width)] if stage == 0 else bufs.at[stage - 1, c]

    def exchange(stage, c):
        return pltpu.make_async_remote_copy(
            src_ref=own(stage, c), dst_ref=got.at[stage, c],
            send_sem=send.at[stage, c], recv_sem=recv.at[stage, c],
            device_id=(partners[stage], blk_no), device_id_type=pl.DeviceIdType.MESH,
        )

    def spread(d, c):
        here = coefs.at[blk_no, pl.ds(c * tiles, tiles)]
        return pltpu.make_async_remote_copy(
            src_ref=here, dst_ref=here,
            send_sem=gsend.at[d - 1, c], recv_sem=grecv.at[d - 1, c],
            device_id=(leaf_no, peers[d - 1]), device_id_type=pl.DeviceIdType.MESH,
        )

    def combine(todo):
        for stage, c in todo:
            exchange(stage, c).wait_recv()
        results = []
        for stage, c in todo:
            pair = jnp.concatenate([own(stage, c)[...], got[stage, c]], axis=0)
            results.append(mm(m_ref[stage, sides[stage]], pair))
        for (stage, c), w in zip(todo, results):
            if stage < bits - 1:
                bufs[stage, c] = w
            else:
                for i in range(tiles):
                    coefs[blk_no, c * tiles + i] = w[:, i * LANES : (i + 1) * LANES]
        for stage, c in todo:
            if stage < bits - 1:
                exchange(stage + 1, c).start()
            else:
                for d in range(1, blocks):
                    spread(d, c).start()

    offsets = 2 * node_offsets(cells) - cells + 1

    def turned(g, factor):
        y = g * factor
        if abs(factor) * (ticks // 2) > 0.5:
            y = y - ((y + MAGIC) - MAGIC)
        return cos_sin_turns(y)

    lane = lax.broadcasted_iota(jnp.int32, (1, LANES), 1)

    def evaluate(tile, carry):
        box = (tile * LANES + lane) * leaves + suffix
        center = box * ticks + ticks // 2
        first = pl.multiple_of(tile * LANES, LANES)
        g_t[...] = (tgt[pl.ds(first, LANES), :].T - center).astype(jnp.float32)

        def chunk(i, carry):
            here = pl.ds(pl.multiple_of(i * rows, rows), rows)
            g = g_t[here, :]
            acc = [[None, None] for _ in range(blocks)]
            for t in range(half):
                c, s = turned(g, float(offsets[t]) * 2.0**-33)
                for q in range(blocks):
                    for part in range(2):
                        sc = coefs[q, tile, pl.ds(part * half + t, 1), :]
                        sd = coefs[q, tile, pl.ds((2 + part) * half + t, 1), :]
                        term = sc * c + sd * s
                        acc[q][part] = term if t == 0 else acc[q][part] + term
            zc, zs = turned(g, float(cells) * 2.0**-32)
            re, im = acc[blocks - 1]
            for q in range(blocks - 2, -1, -1):
                re, im = zc * re - zs * im + acc[q][0], zc * im + zs * re + acc[q][1]
            pc, ps = turned(g, float(cells - 1) * 2.0**-33)
            re_t[here, :] = pc * re - ps * im
            im_t[here, :] = pc * im + ps * re
            return carry

        lax.fori_loop(0, TGT_BOX // rows, chunk, 0)
        out[pl.ds(2 * first, LANES, stride=2), :] = re_t[...].T
        out[pl.ds(2 * first + 1, LANES, stride=2), :] = im_t[...].T
        return carry

    def put(c):
        span = pl.ds(2 * c * width, 2 * width)
        return pltpu.make_async_copy(out.at[span], out_hbm.at[span], osem.at[c])

    def field(c):
        if c == 0:
            fetch.wait()
        for d in range(1, blocks):
            spread(d, c).wait_recv()
        lax.fori_loop(c * tiles, (c + 1) * tiles, evaluate, 0)
        put(c).start()

    ahead = min(3, chunks)
    for c in range(ahead):
        exchange(0, c).start()
    for step in range(chunks + bits):
        combine([(k, step - k) for k in range(bits - 1, -1, -1) if 0 <= step - k < chunks])
        if step + ahead < chunks:
            exchange(0, step + ahead).start()
        if step >= bits:
            field(step - bits)
    for c in range(chunks):
        for stage in range(bits):
            exchange(stage, c).wait_send()
        for d in range(1, blocks):
            spread(d, c).wait_send()
        put(c).wait()


def finish_call(weights, ticks, matrices, leaves, blocks, depth, chunks):
    boxes = ticks.shape[0]
    bits = leaves.bit_length() - 1
    width = boxes // chunks
    whole = pl.BlockSpec(memory_space=pltpu.VMEM)
    anywhere = pl.BlockSpec(memory_space=pl.ANY)
    dma = pltpu.SemaphoreType.DMA
    return pl.pallas_call(
        functools.partial(finish_kernel, leaves=leaves, blocks=blocks, chunks=chunks, depth=depth, rows=16),
        out_shape=jax.ShapeDtypeStruct((2 * boxes, TGT_BOX), jnp.float32),
        in_specs=[whole, anywhere, whole],
        out_specs=anywhere,
        scratch_shapes=[
            pltpu.VMEM((boxes, TGT_BOX), jnp.int32),
            pltpu.VMEM((2 * boxes, TGT_BOX), jnp.float32),
            pltpu.VMEM((bits - 1, chunks, 2 * R, width), jnp.float32),
            pltpu.VMEM((bits, chunks, 2 * R, width), jnp.float32),
            pltpu.VMEM((blocks, boxes // LANES, 2 * R, LANES), jnp.float32),
        ] + [pltpu.VMEM((TGT_BOX, LANES), jnp.float32)] * 3 + [
            dma((bits, chunks)), dma((bits, chunks)),
            dma((blocks - 1, chunks)), dma((blocks - 1, chunks)),
            dma, dma((chunks,)),
        ],
        compiler_params=pltpu.CompilerParams(collective_id=0, has_side_effects=True),
        name="finish",
    )(weights, ticks, matrices)


def table(m):
    return jnp.asarray(m.astype(np.float32))


def mm(a, b):
    return jnp.dot(a, b, precision=HIGHEST, preferred_element_type=jnp.float32)


def local_tree(leaf, boxes):
    low = leaf.shape[0]
    n1 = low.bit_length() - 1
    rest = boxes.bit_length() - 1 - n1
    n2 = rest - rest // 2
    n3 = rest - n2
    c = 2 * R
    y = mm(table(radix_matrix(0, n1)), leaf.reshape(low * c, -1))
    y = y.reshape(low, c, 2**n3, 2**n2).transpose(3, 1, 0, 2).reshape(2**n2 * c, -1)
    y = mm(table(radix_matrix(n1, n2)), y)
    y = y.reshape(2**n2, c, low, 2**n3).transpose(3, 1, 2, 0).reshape(2**n3 * c, -1)
    y = mm(table(radix_matrix(n1 + n2, n3)), y)
    return y.reshape(2**n3, c, low * 2**n2).transpose(1, 2, 0).reshape(c, boxes)


def local(src_pos, strengths, tgt_pos):
    leaf_count = lax.axis_size("leaf")
    leaf_bits = leaf_count.bit_length() - 1
    boxes = src_pos.shape[1] // PER_BOX
    local_depth = boxes.bit_length() - 1
    leaf = leaf_call(src_pos.reshape(boxes, PER_BOX), strengths.reshape(2, boxes, PER_BOX))
    weights = local_tree(leaf, boxes)
    steps = np.stack([step_matrix(local_depth + k) for k in range(leaf_bits)])
    steps[-1] = np.einsum("xy,ejyz->ejxz", fold_pairs(), steps[-1])
    steps[:, 1] = steps[:, 1, ::-1]
    steps = np.concatenate([steps[:, :, 0], steps[:, :, 1]], axis=-1)
    out = finish_call(
        weights, tgt_pos.reshape(boxes, TGT_BOX), table(steps), leaf_count, lax.axis_size("blk"),
        local_depth + leaf_bits, 8,
    )
    return out.reshape(boxes, 2, TGT_BOX).transpose(1, 0, 2).reshape(2, boxes * TGT_BOX)


def solution(mesh):
    return jax.shard_map(
        local,
        mesh=mesh,
        in_specs=(P("blk", "leaf"), P(None, "blk", "leaf"), P(("leaf", "blk"))),
        out_specs=P(None, ("leaf", "blk")),
        check_vma=False,
    )
```
